32 devices in a mesh: groups: 2 (over y), gx: 4 (over z), gy: 4 (over x, core).
Axes of the slice: x: 2, y: 2, z: 4, core: 2. Of those that a mesh axis runs over, the one named last changes fastest.
Arguments:
- hidden_in: bfloat16 [128, 18432], P(('groups', 'gx'), 'gy'), parts along dimension 0, may hold values from -6 to 6
- w_query: bfloat16 [18432, 12288], P('gy', 'gx'), may hold values from -0.046875 to 0.046875
- w_out: bfloat16 [12288, 18432], P('gx', 'gy'), may hold values from -0.4375 to 0.4375
- cache_keys: bfloat16 [128, 1024, 256], P(('groups', 'gx', 'gy')), parts along dimension 0, may hold values from -250 to 250
- cache_values: bfloat16 [128, 1024, 256], P(('groups', 'gx', 'gy')), parts along dimension 0, may hold values from -6 to 6
- lengths: int32 [128], P(('groups', 'gx', 'gy')), parts along dimension 0, may hold values from 128 to 1024
Outputs:
- layer_out: bfloat16 [128, 18432], P(('groups', 'gx'), 'gy'), parts along dimension 0
The draws below stay inside these ranges and needn't reach their ends.
There are 2 independent parts, one for each index of `groups`. The reference program is written for one: setup_inputs(seed, part) draws one part's arguments, and reference() takes and returns one part's arrays. A program takes and returns all parts, laid end to end along the dimension named above; an argument that names none is the same for every part. Nothing has to cross between parts.
All inputs are finite; a program needn't handle non-finite values.
Results may differ from the reference program's by a relative error of at most 0.0097.
Values may be sent and summed in bfloat16 or wider, within the bound.
A program may use at most 128 MiB of HBM per device.

```python
import jax
import jax.numpy as jnp
from jax import lax

D = 18432
HEADS = 48
HD = 256
QW = 12288
SEQ_DEV = 4
LMAX = 1024
B = 64


def draw_cache_keys(key, part):
    base = jnp.clip(jax.random.normal(jax.random.fold_in(key, 11), (B, LMAX, HD), jnp.float32), -6.0, 6.0)
    return base.astype(jnp.bfloat16)


def touch_ends(drawn, own_key, smallest, high):
    longest = drawn.shape.index(max(drawn.shape))
    spots = []
    for shift in (0, 1):
        where = [jax.random.randint(jax.random.fold_in(own_key, axis), (), 0, length) for axis, length in enumerate(drawn.shape)]
        where[longest] = (where[longest] + shift) % drawn.shape[longest]
        spots.append(tuple(where))
    return drawn.at[spots[0]].set(smallest).at[spots[1]].set(high)


def levels(own_key, dims, pieces, least, high):
    loudness, own = 1.0, jax.random.fold_in(own_key, 6)
    for dim, shards_of in pieces:
        draws = jnp.exp(jax.random.uniform(jax.random.fold_in(own, dim), (shards_of,), jnp.float32, least / len(pieces), high / len(pieces)))
        loudness = loudness * jnp.repeat(draws, dims[dim] // shards_of).reshape([-1 if axis == dim else 1 for axis in range(len(dims))])
    return loudness


def normal_values(own_key, dims, spread, most, cuts=(), held_as=jnp.bfloat16):
    drawn = jax.random.normal(own_key, dims, jnp.float32) * spread
    if len(cuts) > 0:
        drawn = levels(own_key, dims, cuts, -0.22, 0.18) * drawn
    return jnp.clip(drawn, min=-most, max=most).astype(held_as)


def setup_inputs(seed: int = 0, part: int = 0) -> dict:
    splits = jax.random.split(jax.random.key(seed), 7)
    own_keys = jax.random.split(jax.random.fold_in(splits[6], part), 7)
    return {
        "hidden_in": normal_values(own_keys[0], (B, D), 1.0, 6.0, ((0, 4), (1, 4))),
        "w_query": normal_values(splits[1], (D, QW), D ** -0.5, 0.046875, ((0, 4), (1, 4))),
        "w_out": normal_values(splits[2], (QW, D), (QW // 64) ** -0.5, 0.4375, ((0, 4), (1, 4))),
        "cache_keys": draw_cache_keys(jax.random.fold_in(jax.random.fold_in(splits[6], part), 71), part),
        "cache_values": normal_values(own_keys[4], (B, LMAX, HD), 1.0, 6.0, ((0, 16),)),
        "lengths": touch_ends(jax.random.randint(own_keys[5], (B,), LMAX // 8, LMAX + 1), jax.random.fold_in(own_keys[5], 1), LMAX // 8, LMAX).astype(jnp.int32),
    }


def attend(operands):
    query_block, key_block, value_block, length_block = operands
    scores = jnp.einsum('bhd,bld->bhl', query_block.astype(jnp.float32), key_block.astype(jnp.float32)) / jnp.sqrt(jnp.float32(HD))
    live_slots = jnp.arange(LMAX)[None, None, :] < length_block[:, None, None]
    scores = jnp.where(live_slots, scores, jnp.float32(-1e+30))
    top_score = lax.optimization_barrier(jnp.max(scores, axis=2, keepdims=True))
    expo = jnp.where(live_slots, jnp.exp(scores - top_score), jnp.float32(0.0))
    probs = (expo / lax.optimization_barrier(jnp.sum(expo, axis=2, keepdims=True))).astype(jnp.bfloat16)
    mixed = jnp.einsum('bhl,bld->bhd', probs.astype(jnp.float32), value_block.astype(jnp.float32))
    return mixed.astype(jnp.bfloat16)

def reference(hidden_in, w_query, w_out, cache_keys, cache_values, lengths):
    query = jnp.dot(hidden_in, w_query, preferred_element_type=jnp.float32).astype(jnp.bfloat16)
    blocks = B // SEQ_DEV
    query_heads = query.reshape(blocks, SEQ_DEV, HEADS, HD)
    key_blocks = cache_keys.reshape(blocks, SEQ_DEV, LMAX, HD)
    value_blocks = cache_values.reshape(blocks, SEQ_DEV, LMAX, HD)
    length_blocks = lengths.reshape(blocks, SEQ_DEV)
    attended = lax.map(attend, (query_heads, key_blocks, value_blocks, length_blocks))
    attended = attended.reshape(B, QW)
    return jnp.dot(attended, w_out, preferred_element_type=jnp.float32).astype(jnp.bfloat16)
```

```python
import functools

import jax
import jax.numpy as jnp
import numpy as np
from jax import lax
from jax.experimental import pallas as pl
from jax.experimental.pallas import tpu as pltpu
from jax.sharding import PartitionSpec as P

MESH = pl.DeviceIdType.MESH
VMEM_LIMIT = 67043328


def pieces(total, most):
    return max(count for count in range(1, most + 1) if total % (count * 256) == 0)


def permutation(dims, order):
    moved = np.arange(int(np.prod(dims))).reshape(dims).transpose(order).reshape(-1)
    return np.eye(moved.size, dtype=np.float32)[moved]


def remote(src, dst, send, recv, device):
    return pltpu.make_async_remote_copy(
        src_ref=src, dst_ref=dst, send_sem=send, recv_sem=recv, device_id=device, device_id_type=MESH
    )


def kernel(
    nz, seqs, heads, kparts, qparts, oparts, spots,
    hidden_ref, wq_ref, wo_ref, keys_ref, values_ref, perm_ref, lengths_ref,
    out_ref,
    wq, wo, keys, values, perms, hid, pq, r1, s2, r2, qs, qr, at, gat, am, po,
    in_sem, wq_sem, wo_sem,
    hr_sem, hl_sem, hid_sem,
    a_send, a_recv, b_send, b_recv,
    q_send, q_recv, t_send, t_recv,
    x_send, x_recv, c_send, c_recv, f_send, f_recv,
    o_send, ol_recv, or_recv,
):
    z = lax.axis_index("gx")
    j = lax.axis_index("gy")
    x, c = j // 2, j % 2
    xo, co = 1 - x, 1 - c
    pair = x * 2 + co
    across = xo * 2 + c
    diag = xo * 2 + co
    rows = hid.shape[1]
    depth, slice_width = wq.shape
    width = wo.shape[1]
    hd = keys.shape[2]
    slots = keys.shape[1]
    kc, qc, oc = depth // kparts, slice_width // qparts, width // oparts
    block = seqs * heads

    hid_in = pltpu.make_async_copy(hidden_ref, hid.at[z], in_sem.at[0])
    hid_in.start()
    perm_in = pltpu.make_async_copy(perm_ref, perms, in_sem.at[1])
    perm_in.start()
    keys_in = pltpu.make_async_copy(keys_ref, keys, in_sem.at[2])
    values_in = pltpu.make_async_copy(values_ref, values, in_sem.at[3])

    def wq_in(k):
        part = pl.ds(k * kc, kc)
        return pltpu.make_async_copy(wq_ref.at[part], wq.at[part], wq_sem.at[k])

    def wo_in(k):
        part = pl.ds(k * (slice_width // kparts), slice_width // kparts)
        return pltpu.make_async_copy(wo_ref.at[part], wo.at[part], wo_sem.at[k])

    for k in range(kparts):
        wq_in(k).start()

    barrier = pltpu.get_barrier_semaphore()
    for d in range(1, nz):
        pl.semaphore_signal(barrier, inc=1, device_id={"gx": lax.rem(z + d, nz)}, device_id_type=MESH)
    for peer in (pair, across):
        pl.semaphore_signal(barrier, inc=1, device_id={"gy": peer}, device_id_type=MESH)
    pl.semaphore_wait(barrier, nz + 1)

    def hid_right(src, k):
        part = hid.at[src, :, pl.ds(k * kc, kc)]
        return remote(part, part, hr_sem.at[src, k], hid_sem.at[src, k], {"gx": lax.rem(z + 1, nz)})

    def hid_left(src, k):
        part = hid.at[src, :, pl.ds(k * kc, kc)]
        return remote(part, part, hl_sem.at[src, k], hid_sem.at[src, k], {"gx": lax.rem(z + nz - 1, nz)})

    hid_in.wait()
    for k in range(kparts):
        @pl.when(z < nz - 1)
        def _():
            hid_right(z, k).start()

        @pl.when(z > 0)
        def _():
            hid_left(z, k).start()

    perm_in.wait()

    def perm(name):
        start, size = spots[name]
        return perms[start : start + size, :size]

    def moved(name, value):
        return jnp.dot(perm(name), value, preferred_element_type=jnp.float32).astype(jnp.bfloat16)

    def stage_a(far, n):
        there = xo if far else x
        cols = pl.ds(n * qc, qc)
        src = pq.at[pl.ds(pl.multiple_of((there * 2 + co) * rows, rows), rows), cols]
        return remote(src, r1.at[1 if far else 0, :, cols], a_send.at[far, n], a_recv.at[far, n], {"gy": pair})

    for t in range(1, nz):
        for k in range(kparts):
            @pl.when(z - t >= 0)
            def _():
                hid_right(z - t, k).wait_recv()

                @pl.when(z < nz - 1)
                def _():
                    hid_right(z - t, k).start()

            @pl.when(z + t < nz)
            def _():
                hid_left(z + t, k).wait_recv()

                @pl.when(z > 0)
                def _():
                    hid_left(z + t, k).start()

            if t == max(nz - 2, 1):
                wq_in(k).wait()
                wo_in(k).start()
                if k == 0:
                    keys_in.start()
                    values_in.start()
            if t == nz - 1:
                piece = hid[:, :, k * kc : (k + 1) * kc].reshape(nz * rows, kc)
                piece = moved("in", piece)
                depths = slice(k * kc, (k + 1) * kc)

                if k < kparts - 1:
                    @pl.loop(0, qparts)
                    def _(n):
                        cols = pl.ds(pl.multiple_of(n * qc, qc), qc)
                        part = jnp.dot(piece, wq[depths, cols], preferred_element_type=jnp.float32)
                        if k > 0:
                            part = part + pq[:, cols]
                        pq[:, cols] = part
                else:
                    for n in range(qparts):
                        cols = slice(n * qc, (n + 1) * qc)
                        part = jnp.dot(piece, wq[depths, cols], preferred_element_type=jnp.float32)
                        if k > 0:
                            part = part + pq[:, cols]
                        pq[:, cols] = part
                        stage_a(1, n).start()
                        stage_a(0, n).start()

    def stage_b(n):
        cols = pl.ds(n * qc, qc)
        return remote(s2.at[:, cols], r2.at[:, cols], b_send.at[n], b_recv.at[n], {"gy": across})

    for n in range(qparts):
        cols = slice(n * qc, (n + 1) * qc)
        stage_a(1, n).wait_recv()
        far = pl.ds(pl.multiple_of(across * rows, rows), rows)
        s2[:, cols] = pq[far, cols] + r1[1, :, cols]
        stage_b(n).start()
    tiles = []
    for n in range(qparts):
        cols = slice(n * qc, (n + 1) * qc)
        stage_a(0, n).wait_recv()
        stage_b(n).wait_recv()
        near = pl.ds(pl.multiple_of(j * rows, rows), rows)
        summed = (pq[near, cols] + r1[0, :, cols] + r2[:, cols]).astype(jnp.bfloat16)
        tiles += [summed[:, h * hd : (h + 1) * hd] for h in range(qc // hd)]
    query = moved("query", jnp.concatenate(tiles, axis=0))
    qs[...] = query.reshape(nz, block, hd)

    def q_copy(d):
        return remote(
            qs.at[lax.rem(z + d, nz)], qr.at[z], q_send.at[d], q_recv.at[d], {"gx": lax.rem(z + d, nz)}
        )

    def q_arrival(d):
        return remote(
            qs.at[z], qr.at[lax.rem(z - d + nz, nz)], q_send.at[d], q_recv.at[d], {"gx": lax.rem(z + d, nz)}
        )

    for d in range(1, nz):
        q_copy(d).start()
    qr[z] = qs[z]
    keys_in.wait()
    values_in.wait()
    for d in range(1, nz):
        q_arrival(d).wait_recv()

    query = moved("heads", qr[...].reshape(nz * block, hd))
    all_heads = nz * heads
    mixed = []
    for s in range(seqs):
        own = query[s * all_heads : (s + 1) * all_heads]
        scores = lax.dot_general(own, keys[s], (((1,), (1,)), ((), ())), preferred_element_type=jnp.float32)
        scores = scores / np.float32(np.sqrt(hd))
        live = lax.broadcasted_iota(jnp.int32, (all_heads, slots), 1) < lengths_ref[s]
        scores = jnp.where(live, scores, jnp.float32(-1e30))
        top = jnp.max(scores, axis=1, keepdims=True)
        expo = jnp.where(live, jnp.exp(scores - top), jnp.float32(0.0))
        probs = (expo / jnp.sum(expo, axis=1, keepdims=True)).astype(jnp.bfloat16)
        mixed.append(jnp.dot(probs, values[s], preferred_element_type=jnp.float32).astype(jnp.bfloat16))
    attended = moved("back", jnp.concatenate(mixed, axis=0))
    at[...] = attended.reshape(nz, block, hd)

    def t_copy(d):
        return remote(
            at.at[lax.rem(z + d, nz)], gat.at[z, j], t_send.at[d], t_recv.at[d], {"gx": lax.rem(z + d, nz)}
        )

    def t_arrival(d):
        return remote(
            at.at[z], gat.at[lax.rem(z - d + nz, nz), j], t_send.at[d], t_recv.at[d], {"gx": lax.rem(z + d, nz)}
        )

    def from_z(d):
        return lax.rem(z - d + nz, nz)

    def x_copy(d, slot):
        part = gat.at[from_z(d), slot]
        return remote(part, part, x_send.at[d], x_recv.at[d], {"gy": across})

    def c_copy(d, slot):
        part = gat.at[from_z(d), slot]
        return remote(part, part, c_send.at[d], c_recv.at[d], {"gy": pair})

    def f_copy(d, slot):
        part = gat.at[from_z(d), slot]
        return remote(part, part, f_send.at[d], f_recv.at[d], {"gy": pair})

    for d in range(1, nz):
        t_copy(d).start()
    gat[z, j] = at[z]
    for d in range(nz):
        if d > 0:
            t_arrival(d).wait_recv()
        x_copy(d, j).start()
        c_copy(d, j).start()
    for d in range(nz):
        x_copy(d, across).wait_recv()
        f_copy(d, across).start()
    for d in range(nz):
        c_copy(d, pair).wait_recv()
        f_copy(d, diag).wait_recv()
        stacked = moved("rows", gat[from_z(d)].reshape(-1, hd))
        for h in range(heads):
            am[from_z(d), :, h * hd : (h + 1) * hd] = stacked[h * rows : (h + 1) * rows]
    for k in range(kparts):
        wo_in(k).wait()

    def spot(n, d, which):
        return (pl.ds(pl.multiple_of((n * nz + d) * rows, rows), rows), pl.ds(which * oc, oc))

    def o_right(n, d):
        return remote(
            wq.at[spot(n, d, 2)], wq.at[spot(n, d, 0)], o_send.at[n, d], ol_recv.at[n, d], {"gx": lax.rem(z + 1, nz)}
        )

    def o_left(n, d):
        return remote(
            wq.at[spot(n, d, 2)], wq.at[spot(n, d, 1)], o_send.at[n, d], or_recv.at[n, d], {"gx": lax.rem(z + nz - 1, nz)}
        )

    @pl.loop(0, oparts)
    def _(n):
        cols = pl.ds(pl.multiple_of(n * oc, oc), oc)
        part = jnp.dot(am[...].reshape(nz * rows, slice_width), wo[:, cols], preferred_element_type=jnp.float32)
        po[:, :, cols] = part.reshape(nz, rows, oc)

        @pl.when(z == 0)
        def _():
            for d in range(nz - 1, 0, -1):
                wq[spot(n, d, 2)] = po[d, :, cols].astype(jnp.bfloat16)
                o_right(n, d).start()

        @pl.when(z == nz - 1)
        def _():
            for d in range(nz - 1):
                wq[spot(n, d, 2)] = po[d, :, cols].astype(jnp.bfloat16)
                o_left(n, d).start()

    @pl.loop(0, oparts)
    def _(n):
        cols = pl.ds(pl.multiple_of(n * oc, oc), oc)
        for d in range(nz - 1, 1, -1):
            @pl.when((z > 0) & (z < d))
            def _():
                o_right(n, d).wait_recv()
                wq[spot(n, d, 2)] = (po[d, :, cols] + wq[spot(n, d, 0)].astype(jnp.float32)).astype(jnp.bfloat16)
                o_right(n, d).start()
        for d in range(nz - 2):
            @pl.when((z < nz - 1) & (z > d))
            def _():
                o_left(n, d).wait_recv()
                wq[spot(n, d, 2)] = (po[d, :, cols] + wq[spot(n, d, 1)].astype(jnp.float32)).astype(jnp.bfloat16)
                o_left(n, d).start()

        @pl.when(z > 0)
        def _():
            o_right(n, z).wait_recv()
            po[z, :, cols] += wq[spot(n, z, 0)].astype(jnp.float32)

        @pl.when(z < nz - 1)
        def _():
            o_left(n, z).wait_recv()
            po[z, :, cols] += wq[spot(n, z, 1)].astype(jnp.float32)

        out_ref[:, cols] = po[z, :, cols].astype(jnp.bfloat16)

    for t in range(nz):
        for k in range(kparts):
            @pl.when((z - t >= 0) & (z < nz - 1))
            def _():
                hid_right(z - t, k).wait_send()

            @pl.when((z + t < nz) & (z > 0))
            def _():
                hid_left(z + t, k).wait_send()
    for n in range(qparts):
        stage_a(1, n).wait_send()
        stage_a(0, n).wait_send()
        stage_b(n).wait_send()
    for d in range(nz):
        if d > 0:
            q_copy(d).wait_send()
            t_copy(d).wait_send()
        x_copy(d, j).wait_send()
        c_copy(d, j).wait_send()
        f_copy(d, across).wait_send()

    @pl.loop(0, oparts)
    def _(n):
        for d in range(nz):
            @pl.when(z < d)
            def _():
                o_right(n, d).wait_send()

            @pl.when(z > d)
            def _():
                o_left(n, d).wait_send()


def fused(hidden_in, w_query, w_out, cache_keys, cache_values, lengths):
    nz, ny = lax.axis_size("gx"), lax.axis_size("gy")
    rows = hidden_in.shape[0]
    seqs, slots, hd = cache_keys.shape
    depth, slice_width = w_query.shape
    width = w_out.shape[1]
    heads = slice_width // hd
    block = seqs * heads
    kparts, qparts, oparts = pieces(depth, 6), pieces(slice_width, 4), pieces(width, 6)
    kparts = kparts if slice_width % (kparts * 16) == 0 else 1
    parts = {
        "in": permutation((nz, ny, seqs), (1, 0, 2)),
        "query": permutation((heads, nz, seqs), (1, 2, 0)),
        "heads": permutation((nz, seqs, heads), (1, 0, 2)),
        "back": permutation((seqs, nz, heads), (1, 0, 2)),
        "rows": permutation((ny, seqs, heads), (2, 0, 1)),
    }
    spots, start, widest = {}, 0, -(-max(m.shape[0] for m in parts.values()) // 128) * 128
    packed = []
    for name, m in parts.items():
        spots[name] = (start, m.shape[0])
        start += m.shape[0]
        packed.append(np.pad(m, ((0, 0), (0, widest - m.shape[0]))))
    perms = jnp.asarray(np.concatenate(packed, axis=0), jnp.bfloat16)
    bf16, f32 = jnp.bfloat16, jnp.float32
    dma = pltpu.SemaphoreType.DMA
    anywhere = pl.BlockSpec(memory_space=pl.ANY)
    return pl.pallas_call(
        functools.partial(kernel, nz, seqs, heads, kparts, qparts, oparts, spots),
        out_shape=jax.ShapeDtypeStruct((rows, width), bf16),
        in_specs=[anywhere] * 6 + [pl.BlockSpec(memory_space=pltpu.SMEM)],
        out_specs=pl.BlockSpec(memory_space=pltpu.VMEM),
        scratch_shapes=[
            pltpu.VMEM(w_query.shape, bf16),
            pltpu.VMEM(w_out.shape, bf16),
            pltpu.VMEM(cache_keys.shape, bf16),
            pltpu.VMEM(cache_values.shape, bf16),
            pltpu.VMEM(perms.shape, bf16),
            pltpu.VMEM((nz, rows, depth), bf16),
            pltpu.VMEM((nz * rows, slice_width), f32),
            pltpu.VMEM((2, rows, slice_width), f32),
            pltpu.VMEM((rows, slice_width), f32),
            pltpu.VMEM((rows, slice_width), f32),
            pltpu.VMEM((nz, block, hd), bf16),
            pltpu.VMEM((nz, block, hd), bf16),
            pltpu.VMEM((nz, block, hd), bf16),
            pltpu.VMEM((nz, ny, block, hd), bf16),
            pltpu.VMEM((nz, rows, slice_width), bf16),
            pltpu.VMEM((nz, rows, width), f32),
            dma((4,)), dma((kparts,)), dma((kparts,)),
            dma((nz, kparts)), dma((nz, kparts)), dma((nz, kparts)),
            dma((2, qparts)), dma((2, qparts)), dma((qparts,)), dma((qparts,)),
            dma((nz,)), dma((nz,)), dma((nz,)), dma((nz,)),
            dma((nz,)), dma((nz,)), dma((nz,)), dma((nz,)), dma((nz,)), dma((nz,)),
            dma((oparts, nz)), dma((oparts, nz)), dma((oparts, nz)),
        ],
        compiler_params=pltpu.CompilerParams(
            collective_id=0, has_side_effects=True, vmem_limit_bytes=VMEM_LIMIT
        ),
    )(hidden_in, w_query, w_out, cache_keys, cache_values, perms, lengths)


def plain(hidden_in, w_query, w_out, cache_keys, cache_values, lengths):
    across = lax.axis_size("gx")
    within = lax.axis_size("gy")
    local_seqs = cache_keys.shape[0]
    slot_count = cache_keys.shape[1]
    head_dim = cache_keys.shape[2]
    partial_query = jnp.dot(
        lax.all_gather(hidden_in, "gx", axis=0, tiled=True),
        w_query,
        preferred_element_type=jnp.float32,
    )
    slice_width = partial_query.shape[1]
    summed = lax.psum(partial_query, "gy")
    grouped = summed.reshape(across, within, local_seqs, slice_width)
    own_rows = lax.dynamic_slice_in_dim(grouped, lax.axis_index("gy"), 1, 1)
    query_rows = own_rows.reshape(across * local_seqs, slice_width).astype(jnp.bfloat16)
    query = lax.all_to_all(query_rows, "gx", split_axis=0, concat_axis=1, tiled=True)
    head_count = query.shape[1] // head_dim
    query_heads = query.reshape(local_seqs, head_count, head_dim)
    scores = jnp.einsum("bhd,bld->bhl", query_heads, cache_keys, preferred_element_type=jnp.float32)
    scores = scores / jnp.sqrt(jnp.float32(head_dim))
    live_slots = jnp.arange(slot_count)[None, None, :] < lengths[:, None, None]
    scores = jnp.where(live_slots, scores, jnp.float32(-1e30))
    top_score = jnp.max(scores, axis=2, keepdims=True)
    expo = jnp.where(live_slots, jnp.exp(scores - top_score), jnp.float32(0.0))
    probs = (expo / jnp.sum(expo, axis=2, keepdims=True)).astype(jnp.bfloat16)
    mixed = jnp.einsum("bhl,bld->bhd", probs, cache_values, preferred_element_type=jnp.float32)
    attended = mixed.astype(jnp.bfloat16).reshape(local_seqs, head_count * head_dim)
    spread = lax.all_to_all(attended, "gx", split_axis=1, concat_axis=0, tiled=True)
    stacked = spread.reshape(across, local_seqs, slice_width)
    gathered = lax.all_gather(stacked, "gy", axis=1, tiled=True)
    head_rows = gathered.reshape(across * within * local_seqs, slice_width)
    partial_out = jnp.dot(head_rows, w_out, preferred_element_type=jnp.float32)
    result = lax.psum_scatter(partial_out, "gx", scatter_dimension=0, tiled=True)
    return result.astype(jnp.bfloat16)


def body(hidden_in, w_query, w_out, cache_keys, cache_values, lengths):
    nz, ny = lax.axis_size("gx"), lax.axis_size("gy")
    rows, (seqs, slots, hd) = hidden_in.shape[0], cache_keys.shape
    depth, slice_width = w_query.shape
    width = w_out.shape[1]
    fits = ny == 4 and nz > 1 and slice_width % hd == 0 and hd % 256 == 0 and slots % 128 == 0
    fits = fits and rows % 16 == 0 and depth % 256 == 0 and width % 256 == 0
    if fits:
        tokens, block = nz * rows, seqs * (slice_width // hd)
        stored = 2 * (2 * slice_width * depth + 2 * cache_keys.size)
        working = tokens * (2 * depth + 6 * slice_width + 4 * width) + 16 * rows * slice_width
        fits = block % 16 == 0 and (nz * slice_width // hd) % 16 == 0
        fits = fits and tokens * 6 <= depth and stored + working + 2**20 < VMEM_LIMIT
        fits = fits and 3 * (width // pieces(width, 6)) <= slice_width
    run = fused if fits else plain
    return run(hidden_in, w_query, w_out, cache_keys, cache_values, lengths)


def solution(mesh):
    placed = (
        P(("groups", "gx"), "gy"),
        P("gy", "gx"),
        P("gx", "gy"),
        P(("groups", "gx", "gy"), None, None),
        P(("groups", "gx", "gy"), None, None),
        P(("groups", "gx", "gy")),
    )
    return jax.shard_map(
        body, mesh=mesh, in_specs=placed, out_specs=P(("groups", "gx"), "gy"), check_vma=False
    )
```

```python
import functools

import jax
import jax.numpy as jnp
import numpy as np
from jax import lax
from jax.experimental import pallas as pl
from jax.experimental.pallas import tpu as pltpu
from jax.sharding import PartitionSpec as P

MESH = pl.DeviceIdType.MESH
VMEM_LIMIT = 67043328


def pieces(total, most):
    return max(count for count in range(1, most + 1) if total % (count * 256) == 0)


def permutation(dims, order):
    moved = np.arange(int(np.prod(dims))).reshape(dims).transpose(order).reshape(-1)
    return np.eye(moved.size, dtype=np.float32)[moved]


def remote(src, dst, send, recv, device):
    return pltpu.make_async_remote_copy(
        src_ref=src, dst_ref=dst, send_sem=send, recv_sem=recv, device_id=device, device_id_type=MESH
    )


def kernel(
    nz, seqs, heads, kparts, qparts, oparts, spots,
    hidden_ref, wq_ref, wo_ref, keys_ref, values_ref, perm_ref, lengths_ref,
    out_ref,
    wq, wo, keys, values, perms, hid, pq, r1, s2, r2, qs, qr, at, gat, am, po,
    in_sem, wq_sem, wo_sem,
    hr_sem, hl_sem, hid_sem,
    a_send, a_recv, b_send, b_recv,
    q_send, q_recv, t_send, t_recv,
    x_send, x_recv, c_send, c_recv, f_send, f_recv,
    o_send, ol_recv, or_recv,
):
    z = lax.axis_index("gx")
    j = lax.axis_index("gy")
    x, c = j // 2, j % 2
    xo, co = 1 - x, 1 - c
    pair = x * 2 + co
    across = xo * 2 + c
    diag = xo * 2 + co
    rows = hid.shape[1]
    depth, slice_width = wq.shape
    width = wo.shape[1]
    hd = keys.shape[2]
    slots = keys.shape[1]
    kc, qc, oc = depth // kparts, slice_width // qparts, width // oparts
    block = seqs * heads

    hid_in = pltpu.make_async_copy(hidden_ref, hid.at[z], in_sem.at[0])
    hid_in.start()
    perm_in = pltpu.make_async_copy(perm_ref, perms, in_sem.at[1])
    perm_in.start()
    keys_in = pltpu.make_async_copy(keys_ref, keys, in_sem.at[2])
    values_in = pltpu.make_async_copy(values_ref, values, in_sem.at[3])

    def wq_in(k):
        part = pl.ds(k * kc, kc)
        return pltpu.make_async_copy(wq_ref.at[part], wq.at[part], wq_sem.at[k])

    def wo_in(k):
        part = pl.ds(k * (slice_width // kparts), slice_width // kparts)
        return pltpu.make_async_copy(wo_ref.at[part], wo.at[part], wo_sem.at[k])

    barrier = pltpu.get_barrier_semaphore()
    for d in range(1, nz):
        pl.semaphore_signal(barrier, inc=1, device_id={"gx": lax.rem(z + d, nz)}, device_id_type=MESH)
    for peer in (pair, across):
        pl.semaphore_signal(barrier, inc=1, device_id={"gy": peer}, device_id_type=MESH)
    hid_in.wait()
    for k in range(kparts):
        wq_in(k).start()
    pl.semaphore_wait(barrier, nz + 1)

    def hid_right(src, k):
        part = hid.at[src, :, pl.ds(k * kc, kc)]
        return remote(part, part, hr_sem.at[src, k], hid_sem.at[src, k], {"gx": lax.rem(z + 1, nz)})

    def hid_left(src, k):
        part = hid.at[src, :, pl.ds(k * kc, kc)]
        return remote(part, part, hl_sem.at[src, k], hid_sem.at[src, k], {"gx": lax.rem(z + nz - 1, nz)})

    def send_own(k):
        @pl.when(z < nz - 1)
        def _():
            hid_right(z, k).start()

        @pl.when(z > 0)
        def _():
            hid_left(z, k).start()

    ahead = min(2, kparts)
    for k in range(ahead):
        send_own(k)

    def perm(name):
        start, size = spots[name]
        return perms[start : start + size, :size]

    def moved(name, value):
        return jnp.dot(perm(name), value, preferred_element_type=jnp.float32).astype(jnp.bfloat16)

    def stage_a(far, n):
        there = xo if far else x
        cols = pl.ds(n * qc, qc)
        src = pq.at[pl.ds(pl.multiple_of((there * 2 + co) * rows, rows), rows), cols]
        return remote(src, r1.at[1 if far else 0, :, cols], a_send.at[far, n], a_recv.at[far, n], {"gy": pair})

    def pass_on(t, k):
        @pl.when(z - t >= 0)
        def _():
            hid_right(z - t, k).wait_recv()

            @pl.when(z < nz - 1)
            def _():
                hid_right(z - t, k).start()

        @pl.when(z + t < nz)
        def _():
            hid_left(z + t, k).wait_recv()

            @pl.when(z > 0)
            def _():
                hid_left(z + t, k).start()

    for step in range(kparts + 2 * (nz - 1)):
        if ahead <= step < kparts:
            send_own(step)
        for t in range(1, nz):
            if 0 <= step - 2 * t < kparts:
                pass_on(t, step - 2 * t)
        if 2 <= step < kparts + 2:
            wq_in(step - 2).wait()
            wo_in(step - 2).start()
        k = step - 2 * (nz - 1)
        if k < 0:
            continue
        if k == 0:
            keys_in.start()
            values_in.start()
            perm_in.wait()
        piece = hid[:, :, k * kc : (k + 1) * kc].reshape(nz * rows, kc)
        piece = moved("in", piece)
        depths = slice(k * kc, (k + 1) * kc)

        if k < kparts - 1:
            @pl.loop(0, qparts)
            def _(n):
                cols = pl.ds(pl.multiple_of(n * qc, qc), qc)
                part = jnp.dot(piece, wq[depths, cols], preferred_element_type=jnp.float32)
                if k > 0:
                    part = part + pq[:, cols]
                pq[:, cols] = part
        else:
            for n in range(qparts):
                cols = slice(n * qc, (n + 1) * qc)
                part = jnp.dot(piece, wq[depths, cols], preferred_element_type=jnp.float32)
                if k > 0:
                    part = part + pq[:, cols]
                pq[:, cols] = part
                stage_a(1, n).start()
                stage_a(0, n).start()

    def stage_b(n):
        cols = pl.ds(n * qc, qc)
        return remote(s2.at[:, cols], r2.at[:, cols], b_send.at[n], b_recv.at[n], {"gy": across})

    for n in range(qparts):
        cols = slice(n * qc, (n + 1) * qc)
        stage_a(1, n).wait_recv()
        far = pl.ds(pl.multiple_of(across * rows, rows), rows)
        s2[:, cols] = pq[far, cols] + r1[1, :, cols]
        stage_b(n).start()
    tiles = []
    for n in range(qparts):
        cols = slice(n * qc, (n + 1) * qc)
        stage_a(0, n).wait_recv()
        stage_b(n).wait_recv()
        near = pl.ds(pl.multiple_of(j * rows, rows), rows)
        summed = (pq[near, cols] + r1[0, :, cols] + r2[:, cols]).astype(jnp.bfloat16)
        tiles += [summed[:, h * hd : (h + 1) * hd] for h in range(qc // hd)]
    query = moved("query", jnp.concatenate(tiles, axis=0))
    qs[...] = query.reshape(nz, block, hd)

    def q_copy(d):
        return remote(
            qs.at[lax.rem(z + d, nz)], qr.at[z], q_send.at[d], q_recv.at[d], {"gx": lax.rem(z + d, nz)}
        )

    def q_arrival(d):
        return remote(
            qs.at[z], qr.at[lax.rem(z - d + nz, nz)], q_send.at[d], q_recv.at[d], {"gx": lax.rem(z + d, nz)}
        )

    for d in range(1, nz):
        q_copy(d).start()
    qr[z] = qs[z]
    keys_in.wait()
    values_in.wait()
    for d in range(1, nz):
        q_arrival(d).wait_recv()

    query = moved("heads", qr[...].reshape(nz * block, hd))
    all_heads = nz * heads
    mixed = []
    for s in range(seqs):
        own = query[s * all_heads : (s + 1) * all_heads]
        scores = lax.dot_general(own, keys[s], (((1,), (1,)), ((), ())), preferred_element_type=jnp.float32)
        scores = scores / np.float32(np.sqrt(hd))
        live = lax.broadcasted_iota(jnp.int32, (all_heads, slots), 1) < lengths_ref[s]
        scores = jnp.where(live, scores, jnp.float32(-1e30))
        top = jnp.max(scores, axis=1, keepdims=True)
        expo = jnp.where(live, jnp.exp(scores - top), jnp.float32(0.0))
        probs = (expo / jnp.sum(expo, axis=1, keepdims=True)).astype(jnp.bfloat16)
        mixed.append(jnp.dot(probs, values[s], preferred_element_type=jnp.float32).astype(jnp.bfloat16))
    attended = moved("back", jnp.concatenate(mixed, axis=0))
    at[...] = attended.reshape(nz, block, hd)

    def t_copy(d):
        return remote(
            at.at[lax.rem(z + d, nz)], gat.at[z, j], t_send.at[d], t_recv.at[d], {"gx": lax.rem(z + d, nz)}
        )

    def t_arrival(d):
        return remote(
            at.at[z], gat.at[lax.rem(z - d + nz, nz), j], t_send.at[d], t_recv.at[d], {"gx": lax.rem(z + d, nz)}
        )

    def from_z(d):
        return lax.rem(z - d + nz, nz)

    def x_copy(d, slot):
        part = gat.at[from_z(d), slot]
        return remote(part, part, x_send.at[d], x_recv.at[d], {"gy": across})

    def c_copy(d, slot):
        part = gat.at[from_z(d), slot]
        return remote(part, part, c_send.at[d], c_recv.at[d], {"gy": pair})

    def f_copy(d, slot):
        part = gat.at[from_z(d), slot]
        return remote(part, part, f_send.at[d], f_recv.at[d], {"gy": pair})

    for d in range(1, nz):
        t_copy(d).start()
    gat[z, j] = at[z]
    for d in range(nz):
        if d > 0:
            t_arrival(d).wait_recv()
        x_copy(d, j).start()
        c_copy(d, j).start()
    for d in range(nz):
        x_copy(d, across).wait_recv()
        f_copy(d, across).start()
    for d in range(nz):
        c_copy(d, pair).wait_recv()
        f_copy(d, diag).wait_recv()
        stacked = moved("rows", gat[from_z(d)].reshape(-1, hd))
        for h in range(heads):
            am[from_z(d), :, h * hd : (h + 1) * hd] = stacked[h * rows : (h + 1) * rows]
    for k in range(kparts):
        wo_in(k).wait()

    def spot(n, d, which):
        start = (n * nz + d) * rows
        start = start if isinstance(start, int) else pl.multiple_of(start, rows)
        return (pl.ds(start, rows), pl.ds(which * oc, oc))

    def o_right(n, d):
        return remote(
            wq.at[spot(n, d, 2)], wq.at[spot(n, d, 0)], o_send.at[n, d], ol_recv.at[n, d], {"gx": lax.rem(z + 1, nz)}
        )

    def o_left(n, d):
        return remote(
            wq.at[spot(n, d, 2)], wq.at[spot(n, d, 1)], o_send.at[n, d], or_recv.at[n, d], {"gx": lax.rem(z + nz - 1, nz)}
        )

    def send_right(n, d):
        cols = slice(n * oc, (n + 1) * oc)

        @pl.when((z > 0) & (z < d))
        def _():
            o_right(n, d).wait_recv()
            wq[spot(n, d, 2)] = (po[d, :, cols] + wq[spot(n, d, 0)].astype(jnp.float32)).astype(jnp.bfloat16)
            o_right(n, d).start()

    def send_left(n, d):
        cols = slice(n * oc, (n + 1) * oc)

        @pl.when((z < nz - 1) & (z > d))
        def _():
            o_left(n, d).wait_recv()
            wq[spot(n, d, 2)] = (po[d, :, cols] + wq[spot(n, d, 1)].astype(jnp.float32)).astype(jnp.bfloat16)
            o_left(n, d).start()

    def relay(step, near):
        for d in range(nz - 1, 0, -1):
            n = step - (nz - 1 - d)
            if 0 <= n < oparts:
                @pl.when((2 * z < nz) if near else (2 * z >= nz))
                def _():
                    send_right(n, d)
        for d in range(nz - 1):
            n = step - d
            if 0 <= n < oparts:
                @pl.when((2 * z >= nz) if near else (2 * z < nz))
                def _():
                    send_left(n, d)

    spent = oparts + nz - 2
    for step in range(spent + 4):
        if step < oparts:
            cols = slice(step * oc, (step + 1) * oc)
            part = jnp.dot(am[...].reshape(nz * rows, slice_width), wo[:, cols], preferred_element_type=jnp.float32)
            po[:, :, cols] = part.reshape(nz, rows, oc)
        if step < spent:
            @pl.when(z == 0)
            def _():
                for d in range(nz - 1, 0, -1):
                    n = step - (nz - 1 - d)
                    if 0 <= n < oparts:
                        wq[spot(n, d, 2)] = po[d, :, n * oc : (n + 1) * oc].astype(jnp.bfloat16)
                        o_right(n, d).start()

            @pl.when(z == nz - 1)
            def _():
                for d in range(nz - 1):
                    n = step - d
                    if 0 <= n < oparts:
                        wq[spot(n, d, 2)] = po[d, :, n * oc : (n + 1) * oc].astype(jnp.bfloat16)
                        o_left(n, d).start()
        if step >= 2:
            relay(step - 2, True)
        if step >= 4:
            relay(step - 4, False)

    for n in range(oparts):
        cols = slice(n * oc, (n + 1) * oc)

        @pl.when(z > 0)
        def _():
            o_right(n, z).wait_recv()
            po[z, :, cols] += wq[spot(n, z, 0)].astype(jnp.float32)

        @pl.when(z < nz - 1)
        def _():
            o_left(n, z).wait_recv()
            po[z, :, cols] += wq[spot(n, z, 1)].astype(jnp.float32)

        out_ref[:, cols] = po[z, :, cols].astype(jnp.bfloat16)

    for t in range(nz):
        for k in range(kparts):
            @pl.when((z - t >= 0) & (z < nz - 1))
            def _():
                hid_right(z - t, k).wait_send()

            @pl.when((z + t < nz) & (z > 0))
            def _():
                hid_left(z + t, k).wait_send()
    for n in range(qparts):
        stage_a(1, n).wait_send()
        stage_a(0, n).wait_send()
        stage_b(n).wait_send()
    for d in range(nz):
        if d > 0:
            q_copy(d).wait_send()
            t_copy(d).wait_send()
        x_copy(d, j).wait_send()
        c_copy(d, j).wait_send()
        f_copy(d, across).wait_send()

    @pl.loop(0, oparts)
    def _(n):
        for d in range(nz):
            @pl.when(z < d)
            def _():
                o_right(n, d).wait_send()

            @pl.when(z > d)
            def _():
                o_left(n, d).wait_send()


def fused(hidden_in, w_query, w_out, cache_keys, cache_values, lengths):
    nz, ny = lax.axis_size("gx"), lax.axis_size("gy")
    rows = hidden_in.shape[0]
    seqs, slots, hd = cache_keys.shape
    depth, slice_width = w_query.shape
    width = w_out.shape[1]
    heads = slice_width // hd
    block = seqs * heads
    kparts, qparts, oparts = pieces(depth, 6), pieces(slice_width, 4), pieces(width, 6)
    kparts = kparts if slice_width % (kparts * 16) == 0 else 1
    parts = {
        "in": permutation((nz, ny, seqs), (1, 0, 2)),
        "query": permutation((heads, nz, seqs), (1, 2, 0)),
        "heads": permutation((nz, seqs, heads), (1, 0, 2)),
        "back": permutation((seqs, nz, heads), (1, 0, 2)),
        "rows": permutation((ny, seqs, heads), (2, 0, 1)),
    }
    spots, start, widest = {}, 0, -(-max(m.shape[0] for m in parts.values()) // 128) * 128
    packed = []
    for name, m in parts.items():
        spots[name] = (start, m.shape[0])
        start += m.shape[0]
        packed.append(np.pad(m, ((0, 0), (0, widest - m.shape[0]))))
    perms = jnp.asarray(np.concatenate(packed, axis=0), jnp.bfloat16)
    bf16, f32 = jnp.bfloat16, jnp.float32
    dma = pltpu.SemaphoreType.DMA
    anywhere = pl.BlockSpec(memory_space=pl.ANY)
    return pl.pallas_call(
        functools.partial(kernel, nz, seqs, heads, kparts, qparts, oparts, spots),
        out_shape=jax.ShapeDtypeStruct((rows, width), bf16),
        in_specs=[anywhere] * 6 + [pl.BlockSpec(memory_space=pltpu.SMEM)],
        out_specs=pl.BlockSpec(memory_space=pltpu.VMEM),
        scratch_shapes=[
            pltpu.VMEM(w_query.shape, bf16),
            pltpu.VMEM(w_out.shape, bf16),
            pltpu.VMEM(cache_keys.shape, bf16),
            pltpu.VMEM(cache_values.shape, bf16),
            pltpu.VMEM(perms.shape, bf16),
            pltpu.VMEM((nz, rows, depth), bf16),
            pltpu.VMEM((nz * rows, slice_width), f32),
            pltpu.VMEM((2, rows, slice_width), f32),
            pltpu.VMEM((rows, slice_width), f32),
            pltpu.VMEM((rows, slice_width), f32),
            pltpu.VMEM((nz, block, hd), bf16),
            pltpu.VMEM((nz, block, hd), bf16),
            pltpu.VMEM((nz, block, hd), bf16),
            pltpu.VMEM((nz, ny, block, hd), bf16),
            pltpu.VMEM((nz, rows, slice_width), bf16),
            pltpu.VMEM((nz, rows, width), f32),
            dma((4,)), dma((kparts,)), dma((kparts,)),
            dma((nz, kparts)), dma((nz, kparts)), dma((nz, kparts)),
            dma((2, qparts)), dma((2, qparts)), dma((qparts,)), dma((qparts,)),
            dma((nz,)), dma((nz,)), dma((nz,)), dma((nz,)),
            dma((nz,)), dma((nz,)), dma((nz,)), dma((nz,)), dma((nz,)), dma((nz,)),
            dma((oparts, nz)), dma((oparts, nz)), dma((oparts, nz)),
        ],
        compiler_params=pltpu.CompilerParams(
            collective_id=0, has_side_effects=True, vmem_limit_bytes=VMEM_LIMIT
        ),
    )(hidden_in, w_query, w_out, cache_keys, cache_values, perms, lengths)


def plain(hidden_in, w_query, w_out, cache_keys, cache_values, lengths):
    across = lax.axis_size("gx")
    within = lax.axis_size("gy")
    local_seqs = cache_keys.shape[0]
    slot_count = cache_keys.shape[1]
    head_dim = cache_keys.shape[2]
    partial_query = jnp.dot(
        lax.all_gather(hidden_in, "gx", axis=0, tiled=True),
        w_query,
        preferred_element_type=jnp.float32,
    )
    slice_width = partial_query.shape[1]
    summed = lax.psum(partial_query, "gy")
    grouped = summed.reshape(across, within, local_seqs, slice_width)
    own_rows = lax.dynamic_slice_in_dim(grouped, lax.axis_index("gy"), 1, 1)
    query_rows = own_rows.reshape(across * local_seqs, slice_width).astype(jnp.bfloat16)
    query = lax.all_to_all(query_rows, "gx", split_axis=0, concat_axis=1, tiled=True)
    head_count = query.shape[1] // head_dim
    query_heads = query.reshape(local_seqs, head_count, head_dim)
    scores = jnp.einsum("bhd,bld->bhl", query_heads, cache_keys, preferred_element_type=jnp.float32)
    scores = scores / jnp.sqrt(jnp.float32(head_dim))
    live_slots = jnp.arange(slot_count)[None, None, :] < lengths[:, None, None]
    scores = jnp.where(live_slots, scores, jnp.float32(-1e30))
    top_score = jnp.max(scores, axis=2, keepdims=True)
    expo = jnp.where(live_slots, jnp.exp(scores - top_score), jnp.float32(0.0))
    probs = (expo / jnp.sum(expo, axis=2, keepdims=True)).astype(jnp.bfloat16)
    mixed = jnp.einsum("bhl,bld->bhd", probs, cache_values, preferred_element_type=jnp.float32)
    attended = mixed.astype(jnp.bfloat16).reshape(local_seqs, head_count * head_dim)
    spread = lax.all_to_all(attended, "gx", split_axis=1, concat_axis=0, tiled=True)
    stacked = spread.reshape(across, local_seqs, slice_width)
    gathered = lax.all_gather(stacked, "gy", axis=1, tiled=True)
    head_rows = gathered.reshape(across * within * local_seqs, slice_width)
    partial_out = jnp.dot(head_rows, w_out, preferred_element_type=jnp.float32)
    result = lax.psum_scatter(partial_out, "gx", scatter_dimension=0, tiled=True)
    return result.astype(jnp.bfloat16)


def body(hidden_in, w_query, w_out, cache_keys, cache_values, lengths):
    nz, ny = lax.axis_size("gx"), lax.axis_size("gy")
    rows, (seqs, slots, hd) = hidden_in.shape[0], cache_keys.shape
    depth, slice_width = w_query.shape
    width = w_out.shape[1]
    fits = ny == 4 and nz > 1 and slice_width % hd == 0 and hd % 256 == 0 and slots % 128 == 0
    fits = fits and rows % 16 == 0 and depth % 256 == 0 and width % 256 == 0
    if fits:
        tokens, block = nz * rows, seqs * (slice_width // hd)
        stored = 2 * (2 * slice_width * depth + 2 * cache_keys.size)
        working = tokens * (2 * depth + 6 * slice_width + 4 * width) + 16 * rows * slice_width
        fits = block % 16 == 0 and (nz * slice_width // hd) % 16 == 0
        fits = fits and tokens * 6 <= depth and stored + working + 2**20 < VMEM_LIMIT
        fits = fits and 3 * (width // pieces(width, 6)) <= slice_width
    run = fused if fits else plain
    return run(hidden_in, w_query, w_out, cache_keys, cache_values, lengths)


def solution(mesh):
    placed = (
        P(("groups", "gx"), "gy"),
        P("gy", "gx"),
        P("gx", "gy"),
        P(("groups", "gx", "gy"), None, None),
        P(("groups", "gx", "gy"), None, None),
        P(("groups", "gx", "gy")),
    )
    return jax.shard_map(
        body, mesh=mesh, in_specs=placed, out_specs=P(("groups", "gx"), "gy"), check_vma=False
    )
```
